256 devices in a mesh: pb: 8 (over x, core), pq: 32 (over z, y).
Axes of the slice: x: 4, y: 4, z: 8, core: 2. Of those that a mesh axis runs over, the one named last changes fastest.
Arguments:
- chol_vv: bfloat16 [352, 1792, 1792], P('pb', 'pq'), may hold values from -6 to 6
- chol_ov: bfloat16 [352, 256, 1792], P('pb', 'pq'), may hold values from -6 to 6
- chol_oo: bfloat16 [352, 256, 256], P('pb', 'pq'), may hold values from -6 to 6
- chol_vo: bfloat16 [352, 256, 1792], P('pb', None, 'pq'), may hold values from -6 to 6
- amplitudes: bfloat16 [256, 1792], P(None, 'pq'), may hold values from -0.125 to 0.125
Outputs:
- dressed: bfloat16 [352, 256, 1792], P('pb', 'pq')
- fock_ov: float32 [256, 1792], P('pq')
The draws below stay inside these ranges and needn't reach their ends.
All inputs are finite; a program needn't handle non-finite values.
Results may differ from the reference program's by a relative error of at most 0.0081.
Values may be sent and summed in bfloat16 or wider, within the bound.
No kernel may reach another device: no remote copies, remote signals or barrier semaphores. Data moves between devices by JAX's collectives and lax.ppermute only.
A program may use at most 64 MiB of HBM per device.

```python
import jax
import jax.numpy as jnp
from jax import lax

NOCC = 256
NVIRT = 1792
QB = 44
NQ = 352
N_PB = 8


def levels(rng, dims, cuts, low, top_value):
    loudness, own = 1.0, jax.random.fold_in(rng, 6)
    for dim, shards_of in cuts:
        heights = jnp.exp(jax.random.uniform(jax.random.fold_in(own, dim), (shards_of,), jnp.float32, low / len(cuts), top_value / len(cuts)))
        loudness = loudness * jnp.repeat(heights, dims[dim] // shards_of).reshape([-1 if axis == dim else 1 for axis in range(len(dims))])
    return loudness


def noise(own_key, dims, spread, bound, split=(), dtype=jnp.bfloat16):
    drawn = jax.random.normal(own_key, dims, jnp.float32) * spread
    if len(split) > 0:
        drawn = levels(own_key, dims, split, -0.22, 0.18) * drawn
    return jnp.clip(drawn, min=-bound, max=bound).astype(dtype)


def setup_inputs(seed: int = 0) -> dict:
    splits = jax.random.split(jax.random.key(seed), 6)
    chol_vv = noise(splits[0], (NQ, NVIRT, NVIRT), 1.0, 6.0, ((0, 8), (1, 32)))
    chol_ov = noise(splits[1], (NQ, NOCC, NVIRT), 1.0, 6.0, ((0, 8), (1, 32)))
    chol_oo = noise(splits[2], (NQ, NOCC, NOCC), 1.0, 6.0, ((0, 8), (1, 32)))
    chol_vo = noise(splits[3], (NQ, NOCC, NVIRT), 1.0, 6.0, ((0, 8), (2, 32)))
    amplitudes = noise(splits[4], (NOCC, NVIRT), NVIRT ** -0.5, 0.125, ((1, 32),))
    return {"chol_vv": chol_vv, "chol_ov": chol_ov, "chol_oo": chol_oo, "chol_vo": chol_vo, "amplitudes": amplitudes}


def reference(chol_vv, chol_ov, chol_oo, chol_vo, amplitudes):
    def one_vector(blocks):
        block_vv, block_ov, block_oo, block_vo = blocks
        lprime = (block_oo.astype(jnp.float32) + jnp.dot(block_ov, amplitudes.T, preferred_element_type=jnp.float32)).astype(jnp.bfloat16)
        direct = jnp.dot(amplitudes, block_vv.T, preferred_element_type=jnp.float32)
        occupied = jnp.dot(lprime.T, amplitudes, preferred_element_type=jnp.float32)
        return (block_vo.astype(jnp.float32) + direct - occupied).astype(jnp.bfloat16)

    dressed = lax.map(one_vector, (chol_vv, chol_ov, chol_oo, chol_vo))
    amps_wide = amplitudes.astype(jnp.float32)

    def one_coulomb(block):
        return 2.0 * jnp.sum(block.astype(jnp.float32) * amps_wide)

    coulomb = lax.map(one_coulomb, dressed)

    def add_vector(total, item):
        weight, block = item
        return total + weight * block.astype(jnp.float32), None

    start = jnp.zeros(amplitudes.shape, jnp.float32)
    total, unused = lax.scan(add_vector, start, (coulomb, dressed))
    fock_ov = total / (QB * N_PB)
    return dressed, fock_ov
```

```python
import jax
import jax.numpy as jnp
from jax import lax
from jax.experimental import pallas as pl
from jax.experimental.pallas import tpu as pltpu
from jax.sharding import PartitionSpec as P

NZ, NY = 8, 4
LANES = 128
OWN_I = 8
GROUP = LANES // OWN_I
F32, BF16 = jnp.float32, jnp.bfloat16
NT = (((1,), (1,)), ((), ()))
TN = (((0,), (0,)), ((), ()))


def z_groups():
    return [[z * NY + y for z in range(NZ)] for y in range(NY)]


def y_shift(k):
    return [(z * NY + y, z * NY + (y + k) % NY) for z in range(NZ) for y in range(NY)]


def split3(x):
    hi = x.astype(BF16)
    rest = x - hi.astype(F32)
    mid = rest.astype(BF16)
    low = (rest - mid.astype(F32)).astype(BF16)
    return hi, mid, low


def swap_blocks(tiles):
    lane = lax.broadcasted_iota(jnp.int32, tiles[0].shape, 1)
    bit = 1
    while bit < GROUP:
        upper = (lane // OWN_I) & bit != 0
        out = list(tiles)
        for q in range(GROUP):
            if q & bit:
                continue
            low, high = tiles[q], tiles[q | bit]
            out[q] = jnp.where(upper, pltpu.roll(high, OWN_I * bit, 1), low)
            out[q | bit] = jnp.where(upper, high, pltpu.roll(low, LANES - OWN_I * bit, 1))
        tiles = out
        bit *= 2
    return tiles


def send_side(vv, ov, oo, vo, own, p0, p1, p2, p3, out, tt, d, gram):
    nq, n_own, nocc = vo.shape
    rows = n_own + OWN_I
    full = nq // GROUP * GROUP
    me = lax.axis_index("pq")
    y = me % NY
    for k, piece in enumerate((p0, p1, p2, p3)):
        src = (y - k + NY) % NY
        for z in range(NZ):
            tt[pl.ds(pl.multiple_of((z * NY + src) * n_own, 8), n_own), :] = piece[z]
    amps = tt[...]
    gram[...] = lax.dot_general(amps, amps, TN, preferred_element_type=F32)
    weight = jnp.concatenate(
        [own[...].astype(F32), -gram[pl.ds(pl.multiple_of(me * OWN_I, 8), OWN_I), :]], 0
    )
    lp = jnp.dot(ov[...], amps, preferred_element_type=F32).reshape(nq, OWN_I, nocc)
    d[:, n_own:, :] = (lp + oo[...].astype(F32)).astype(BF16).astype(F32)
    share = []
    for q0 in range(0, nq, GROUP):
        q1 = min(nq, q0 + GROUP)
        part = jnp.dot(vv[q0 * n_own : q1 * n_own, :], amps, preferred_element_type=F32)
        d[q0:q1, :n_own, :] = part.reshape(q1 - q0, n_own, nocc) + vo[q0:q1].astype(F32)
    half = GROUP // 2
    for t in range(nq // GROUP):
        for h in range(nocc // LANES):
            for r in range(0, rows, 16):
                tiles = [
                    d[t * GROUP + q, r : r + 16, h * LANES : (h + 1) * LANES]
                    for q in range(GROUP)
                ]
                for g, tile in enumerate(swap_blocks(tiles)):
                    out[h * GROUP + g, t * rows + r : t * rows + r + 16, :] = tile.astype(BF16)
    left = nq - full
    spare = GROUP - left
    short = rows - 16
    for h in range(nocc // LANES):
        cols = slice(h * LANES, (h + 1) * LANES)
        for n, r in enumerate(range(0, short, 16)):
            tiles = [d[full + q, r : r + 16, cols] for q in range(left)]
            tiles += [d[full + n * spare + v, short:rows, cols] for v in range(spare)]
            for g, tile in enumerate(swap_blocks(tiles)):
                at = full // GROUP * rows + r
                out[h * GROUP + g, at : at + 16, :] = tile.astype(BF16)
    lane = lax.broadcasted_iota(jnp.int32, (1, LANES), 1)
    row = jnp.zeros((1, LANES), F32)
    for q in range(nq):
        total = jnp.sum(d[q] * weight, axis=(0, 1), keepdims=True)
        row = jnp.where(lane == q, 2.0 * total, row)
    block = jnp.concatenate(
        [s.astype(F32) for s in split3(row)] + [jnp.zeros((8 - 3, LANES), F32)], 0
    ).astype(BF16)
    at = full // GROUP * rows + short
    for p in range(out.shape[0]):
        out[p, at : at + 8, :] = block


def receive_side(got, tt, dressed, fock, raw, lpt):
    n_dev = got.shape[0]
    nq = dressed.shape[0] // OWN_I
    nvirt = tt.shape[0]
    n_own = nvirt // n_dev
    rows = n_own + OWN_I
    full = nq // GROUP * GROUP
    n_full = full // GROUP
    left = nq - full
    spare = GROUP - left
    short = rows - 16
    lane16 = lax.broadcasted_iota(jnp.int32, (16, LANES), 1)
    width = spare * OWN_I
    for p in range(n_dev):
        a = p * n_own
        for t in range(n_full):
            raw[a : a + n_own, t * LANES : (t + 1) * LANES] = got[p, t * rows : t * rows + n_own, :]
            lpt[p * OWN_I : (p + 1) * OWN_I, t * LANES : (t + 1) * LANES] = got[
                p, t * rows + n_own : (t + 1) * rows, :
            ]
        base = n_full * rows
        tail = jnp.zeros((16, LANES), F32)
        for n in range(short // 16):
            part = pltpu.roll(
                got[p, base + 16 * n : base + 16 * (n + 1), :].astype(F32), (n + 1) * width, 1
            )
            here = (lane16 >= n * width) & (lane16 < (n + 1) * width)
            tail = jnp.where(here, part, tail)
        raw[a : a + short, n_full * LANES :] = got[p, base : base + short, :]
        raw[a + short : a + n_own, n_full * LANES :] = tail[: n_own - short].astype(BF16)
        lpt[p * OWN_I : (p + 1) * OWN_I, n_full * LANES :] = tail[n_own - short :].astype(BF16)
    lanes_in = (n_full + 1) * LANES
    m = nq * OWN_I
    eye = (
        lax.broadcasted_iota(jnp.int32, (m, lanes_in), 0)
        == lax.broadcasted_iota(jnp.int32, (m, lanes_in), 1)
    ).astype(F32).astype(BF16)
    lp = lax.dot_general(eye, lpt[...], NT, preferred_element_type=F32).astype(BF16)
    moved = lax.dot_general(eye, raw[...], NT, preferred_element_type=F32)
    occupied = lax.dot_general(lp, tt[...], NT, preferred_element_type=F32)
    result = (moved - occupied).astype(BF16)
    dressed[...] = result
    at = n_full * rows + short
    shares = jnp.sum(got[:, at : at + 8, :].astype(F32), axis=0)
    coulomb = shares[0:1] + shares[1:2] + shares[2:3]
    pick = lax.broadcasted_iota(jnp.int32, (m, LANES), 1) == lax.broadcasted_iota(
        jnp.int32, (m, LANES), 0
    ) // OWN_I
    column = jnp.sum(jnp.where(pick, coulomb, 0.0), axis=1, keepdims=True)
    fock[...] = jnp.sum((column * result.astype(F32)).reshape(nq, OWN_I, nvirt), axis=0).astype(
        fock.dtype
    )


VMEM = pl.BlockSpec(memory_space=pltpu.VMEM)
PARAMS = pltpu.CompilerParams(vmem_limit_bytes=56 * 1024 * 1024)


def per_device(chol_vv, chol_ov, chol_oo, chol_vo, amplitudes):
    nq, n_own, nvirt = chol_vv.shape
    nocc = amplitudes.shape[0]
    n_dev = lax.axis_size("pq")
    own = amplitudes.T
    near = lax.all_to_all(
        jnp.broadcast_to(own, (NZ, n_own, nocc)), "pq", 0, 0, axis_index_groups=z_groups(), tiled=True
    )
    pieces = [near] + [lax.ppermute(near, "pq", y_shift(k)) for k in range(1, NY)]
    rows = n_own + OWN_I
    sent_rows = nq * rows * OWN_I // LANES + 8
    sent, tt = pl.pallas_call(
        send_side,
        out_shape=(
            jax.ShapeDtypeStruct((n_dev, sent_rows, LANES), BF16),
            jax.ShapeDtypeStruct((nvirt, nocc), BF16),
        ),
        in_specs=[VMEM] * 9,
        out_specs=(VMEM, VMEM),
        scratch_shapes=[pltpu.VMEM((nq, rows, nocc), F32), pltpu.VMEM((nocc, nocc), F32)],
        compiler_params=PARAMS,
        name="send_side",
    )(
        chol_vv.reshape(nq * n_own, nvirt),
        chol_ov.reshape(nq * OWN_I, nvirt),
        chol_oo,
        chol_vo.transpose(0, 2, 1),
        own,
        *pieces,
    )
    got = lax.all_to_all(sent, "pq", 0, 0, tiled=True)
    lanes_in = -(-nq // GROUP) * LANES
    dressed, fock = pl.pallas_call(
        receive_side,
        out_shape=(
            jax.ShapeDtypeStruct((nq * OWN_I, nvirt), BF16),
            jax.ShapeDtypeStruct((OWN_I, nvirt), BF16),
        ),
        in_specs=[VMEM] * 2,
        out_specs=(VMEM, VMEM),
        scratch_shapes=[pltpu.VMEM((nvirt, lanes_in), BF16), pltpu.VMEM((nocc, lanes_in), BF16)],
        compiler_params=PARAMS,
        name="receive_side",
    )(got, tt)
    n_pb = lax.axis_size("pb")
    parts = lax.all_to_all(jnp.broadcast_to(fock, (n_pb, *fock.shape)), "pb", 0, 0, tiled=True)
    fock_ov = jnp.sum(parts.astype(F32), axis=0) / (nq * n_pb)
    return dressed.reshape(nq, OWN_I, nvirt), fock_ov


def solution(mesh):
    in_specs = (
        P("pb", "pq", None),
        P("pb", "pq", None),
        P("pb", "pq", None),
        P("pb", None, "pq"),
        P(None, "pq"),
    )
    out_specs = (P("pb", "pq", None), P("pq", None))
    return jax.shard_map(
        per_device, mesh=mesh, in_specs=in_specs, out_specs=out_specs, check_vma=False
    )
```

```python
import functools

import jax
import jax.numpy as jnp
from jax import lax
from jax.experimental import pallas as pl
from jax.experimental.pallas import tpu as pltpu
from jax.sharding import PartitionSpec as P

NZ, NY = 8, 4
LANES = 128
OWN_I = 8
GROUP = LANES // OWN_I
F32, BF16 = jnp.float32, jnp.bfloat16
NT = (((1,), (1,)), ((), ()))
TN = (((0,), (0,)), ((), ()))


def z_groups():
    return [[z * NY + y for z in range(NZ)] for y in range(NY)]


def y_shift(k):
    return [(z * NY + y, z * NY + (y + k) % NY) for z in range(NZ) for y in range(NY)]


def split3(x):
    hi = x.astype(BF16)
    rest = x - hi.astype(F32)
    mid = rest.astype(BF16)
    low = (rest - mid.astype(F32)).astype(BF16)
    return hi, mid, low


def swap_blocks(tiles):
    lane = lax.broadcasted_iota(jnp.int32, tiles[0].shape, 1)
    bit = 1
    while bit < GROUP:
        upper = (lane // OWN_I) & bit != 0
        out = list(tiles)
        for q in range(GROUP):
            if q & bit:
                continue
            low, high = tiles[q], tiles[q | bit]
            out[q] = jnp.where(upper, pltpu.roll(high, OWN_I * bit, 1), low)
            out[q | bit] = jnp.where(upper, high, pltpu.roll(low, LANES - OWN_I * bit, 1))
        tiles = out
        bit *= 2
    return tiles


def touch(near, vv, ov, oo, vo, token):
    del near, vv, ov, oo, vo
    token[...] = jnp.zeros_like(token)


def send_side(token, vv, ov, oo, vo, own, *refs):
    del token
    pieces, (out, tt, d, gram) = refs[: 2 * NY], refs[2 * NY :]
    nq, n_own, nocc = vo.shape
    rows = n_own + OWN_I
    full = nq // GROUP * GROUP
    me = lax.axis_index("pq")
    core = lax.axis_index("pb") & 1
    y = me & (NY - 1)
    half = pieces[0].shape[1]
    for k in range(NY):
        src = (y - k + NY) & (NY - 1)
        for c in range(2):
            shift = (core if c == 0 else 1 - core) * (n_own - half)
            for z in range(NZ):
                at = pl.multiple_of((z * NY + src) * n_own + shift, 8)
                tt[pl.ds(at, half), :] = pieces[2 * k + c][z]
    amps = tt[...]
    lp = jnp.dot(ov[...], amps, preferred_element_type=F32).reshape(nq, OWN_I, nocc)
    d[:, n_own:, :] = (lp + oo[...].astype(F32)).astype(BF16).astype(F32)

    def dress(t):
        q0, q1 = t * GROUP, min(nq, (t + 1) * GROUP)
        part = jnp.dot(vv[q0 * n_own : q1 * n_own, :], amps, preferred_element_type=F32)
        d[q0:q1, :n_own, :] = part.reshape(q1 - q0, n_own, nocc) + vo[q0:q1].astype(F32)

    left = nq - full
    spare = GROUP - left
    short = rows - 16

    def pack(t):
        for h in range(nocc // LANES):
            cols = slice(h * LANES, (h + 1) * LANES)
            for r in range(0, rows if t * GROUP < full else short, 8):
                if t * GROUP < full:
                    tiles = [d[t * GROUP + q, r : r + 8, cols] for q in range(GROUP)]
                else:
                    n, r2 = divmod(r, 16)
                    tiles = [d[full + q, r : r + 8, cols] for q in range(left)]
                    tiles += [
                        d[full + n * spare + v, short + r2 : short + r2 + 8, cols]
                        for v in range(spare)
                    ]
                for g, tile in enumerate(swap_blocks(tiles)):
                    out[h * GROUP + g, t * rows + r : t * rows + r + 8, :] = tile.astype(BF16)

    lane = lax.broadcasted_iota(jnp.int32, (1, LANES), 1)
    row = jnp.zeros((1, LANES), F32)
    n_tiles = -(-nq // GROUP)
    dress(0)
    for t in range(1, n_tiles):
        dress(t)
        pack(t - 1)
    gram[...] = lax.dot_general(amps, amps, TN, preferred_element_type=F32)
    pack(n_tiles - 1)
    weight = jnp.concatenate(
        [own[...].astype(F32), -gram[pl.ds(pl.multiple_of(me * OWN_I, 8), OWN_I), :]], 0
    )
    for q in range(nq):
        total = jnp.sum(d[q] * weight, axis=(0, 1), keepdims=True)
        row = jnp.where(lane == q, 2.0 * total, row)
    block = jnp.concatenate(
        [s.astype(F32) for s in split3(row)] + [jnp.zeros((8 - 3, LANES), F32)], 0
    ).astype(BF16)
    at = full // GROUP * rows + short
    for p in range(out.shape[0]):
        out[p, at : at + 8, :] = block


def receive_side(scale, got, tt, dressed, fock, raw, lpt):
    n_dev = got.shape[0]
    nq = dressed.shape[0] // OWN_I
    nvirt = tt.shape[0]
    n_own = nvirt // n_dev
    rows = n_own + OWN_I
    full = nq // GROUP * GROUP
    n_full = full // GROUP
    left = nq - full
    spare = GROUP - left
    short = rows - 16
    lane16 = lax.broadcasted_iota(jnp.int32, (16, LANES), 1)
    width = spare * OWN_I
    for p in range(n_dev):
        a = p * n_own
        for t in range(n_full):
            raw[a : a + n_own, t * LANES : (t + 1) * LANES] = got[p, t * rows : t * rows + n_own, :]
            lpt[p * OWN_I : (p + 1) * OWN_I, t * LANES : (t + 1) * LANES] = got[
                p, t * rows + n_own : (t + 1) * rows, :
            ]
        base = n_full * rows
        tail = jnp.zeros((16, LANES), F32)
        for n in range(short // 16):
            part = pltpu.roll(
                got[p, base + 16 * n : base + 16 * (n + 1), :].astype(F32), (n + 1) * width, 1
            )
            here = (lane16 >= n * width) & (lane16 < (n + 1) * width)
            tail = jnp.where(here, part, tail)
        raw[a : a + short, n_full * LANES :] = got[p, base : base + short, :]
        raw[a + short : a + n_own, n_full * LANES :] = tail[: n_own - short].astype(BF16)
        lpt[p * OWN_I : (p + 1) * OWN_I, n_full * LANES :] = tail[n_own - short :].astype(BF16)
    lanes_in = (n_full + 1) * LANES
    m = nq * OWN_I
    eye = (
        lax.broadcasted_iota(jnp.int32, (m, lanes_in), 0)
        == lax.broadcasted_iota(jnp.int32, (m, lanes_in), 1)
    ).astype(F32).astype(BF16)
    lp = lax.dot_general(eye, lpt[...], NT, preferred_element_type=F32).astype(BF16)
    moved = lax.dot_general(eye, raw[...], NT, preferred_element_type=F32)
    occupied = lax.dot_general(lp, tt[...], NT, preferred_element_type=F32)
    result = (moved - occupied).astype(BF16)
    dressed[...] = result
    at = n_full * rows + short
    shares = jnp.sum(got[:, at : at + 8, :].astype(F32), axis=0)
    coulomb = shares[0:1] + shares[1:2] + shares[2:3]
    pick = lax.broadcasted_iota(jnp.int32, (m, LANES), 1) == lax.broadcasted_iota(
        jnp.int32, (m, LANES), 0
    ) // OWN_I
    column = jnp.sum(jnp.where(pick, coulomb, 0.0), axis=1, keepdims=True)
    part = jnp.sum((column * result.astype(F32)).reshape(nq, OWN_I, nvirt), axis=0) * scale
    for copy in range(fock.shape[0]):
        fock[copy] = part.astype(fock.dtype)


VMEM = pl.BlockSpec(memory_space=pltpu.VMEM)
ANY = pl.BlockSpec(memory_space=pl.ANY)
PARAMS = pltpu.CompilerParams(vmem_limit_bytes=26 * 1024 * 1024)


def per_device(chol_vv, chol_ov, chol_oo, chol_vo, amplitudes):
    nq, n_own, nvirt = chol_vv.shape
    nocc = amplitudes.shape[0]
    n_dev, n_pb = lax.axis_size("pq"), lax.axis_size("pb")
    own = amplitudes.T
    half = -(-n_own // 16) * 8
    core = lax.axis_index("pb") & 1
    mine = jnp.where(core == 0, own[:half], own[n_own - half :])
    near = lax.all_to_all(
        jnp.broadcast_to(mine, (NZ, half, nocc)), "pq", 0, 0, axis_index_groups=z_groups(), tiled=True
    )
    other = [(b, b ^ 1) for b in range(n_pb)]
    pieces = [near]
    for k in range(1, NY):
        pieces.append(lax.ppermute(near, "pq", y_shift(k)))
    pieces = [p for piece in pieces for p in (piece, lax.ppermute(piece, "pb", other))]
    blocks = (
        chol_vv.reshape(nq * n_own, nvirt),
        chol_ov.reshape(nq * OWN_I, nvirt),
        chol_oo,
        chol_vo.transpose(0, 2, 1),
    )
    token = pl.pallas_call(
        touch,
        out_shape=jax.ShapeDtypeStruct((8, LANES), F32),
        in_specs=[ANY] * 5,
        out_specs=VMEM,
        compiler_params=PARAMS,
        cost_estimate=pl.CostEstimate(flops=4_000_000_000, bytes_accessed=0, transcendentals=0),
        name="touch",
    )(near, *blocks)
    rows = n_own + OWN_I
    sent_rows = nq * rows * OWN_I // LANES + 8
    sent, tt = pl.pallas_call(
        send_side,
        out_shape=(
            jax.ShapeDtypeStruct((n_dev, sent_rows, LANES), BF16),
            jax.ShapeDtypeStruct((nvirt, nocc), BF16),
        ),
        in_specs=[ANY] + [VMEM] * (5 + 2 * NY),
        out_specs=(VMEM, VMEM),
        scratch_shapes=[pltpu.VMEM((nq, rows, nocc), F32), pltpu.VMEM((nocc, nocc), F32)],
        compiler_params=PARAMS,
        name="send_side",
    )(token, *blocks, own, *pieces)
    got = lax.all_to_all(sent, "pq", 0, 0, tiled=True)
    lanes_in = -(-nq // GROUP) * LANES
    dressed, fock = pl.pallas_call(
        functools.partial(receive_side, 1.0 / (nq * n_pb)),
        out_shape=(
            jax.ShapeDtypeStruct((nq * OWN_I, nvirt), BF16),
            jax.ShapeDtypeStruct((n_pb, OWN_I, nvirt), BF16),
        ),
        in_specs=[VMEM] * 2,
        out_specs=(VMEM, VMEM),
        scratch_shapes=[pltpu.VMEM((nvirt, lanes_in), BF16), pltpu.VMEM((nocc, lanes_in), BF16)],
        compiler_params=PARAMS,
        name="receive_side",
    )(got, tt)
    parts = lax.all_to_all(fock, "pb", 0, 0, tiled=True)
    fock_ov = jnp.sum(parts.astype(F32), axis=0)
    return dressed.reshape(nq, OWN_I, nvirt), fock_ov


def solution(mesh):
    in_specs = (
        P("pb", "pq", None),
        P("pb", "pq", None),
        P("pb", "pq", None),
        P("pb", None, "pq"),
        P(None, "pq"),
    )
    out_specs = (P("pb", "pq", None), P("pq", None))

    return jax.shard_map(per_device, mesh=mesh, in_specs=in_specs, out_specs=out_specs, check_vma=False)
```

```python
import functools

import jax
import jax.numpy as jnp
from jax import lax
from jax.experimental import pallas as pl
from jax.experimental.pallas import tpu as pltpu
from jax.sharding import PartitionSpec as P

NZ, NY = 8, 4
LANES = 128
OWN_I = 8
GROUP = LANES // OWN_I
F32, BF16 = jnp.float32, jnp.bfloat16
NT = (((1,), (1,)), ((), ()))
TN = (((0,), (0,)), ((), ()))


def z_groups():
    return [[z * NY + y for z in range(NZ)] for y in range(NY)]


def y_shift(k):
    return [(z * NY + y, z * NY + (y + k) % NY) for z in range(NZ) for y in range(NY)]


def split3(x):
    hi = x.astype(BF16)
    rest = x - hi.astype(F32)
    mid = rest.astype(BF16)
    low = (rest - mid.astype(F32)).astype(BF16)
    return hi, mid, low


def swap_blocks(tiles):
    lane = lax.broadcasted_iota(jnp.int32, tiles[0].shape, 1)
    bit = 1
    while bit < GROUP:
        upper = (lane // OWN_I) & bit != 0
        out = list(tiles)
        for q in range(GROUP):
            if q & bit:
                continue
            low, high = tiles[q], tiles[q | bit]
            out[q] = jnp.where(upper, pltpu.roll(high, OWN_I * bit, 1), low)
            out[q | bit] = jnp.where(upper, high, pltpu.roll(low, LANES - OWN_I * bit, 1))
        tiles = out
        bit *= 2
    return tiles


def spread(own, out):
    half = out.shape[1]
    start = (lax.axis_index("pb") & 1) * (own.shape[0] - half)
    part = own[pl.ds(pl.multiple_of(start, 8), half), :]
    for copy in range(out.shape[0]):
        out[copy] = part


def touch(near, vv, ov, oo, vo, token):
    del near, vv, ov, oo, vo
    token[...] = jnp.zeros_like(token)


def send_side(token, vv, ov, oo, vo, own, *refs):
    del token
    pieces, (out, tt, d, gram) = refs[: 2 * NY], refs[2 * NY :]
    nq, n_own, nocc = vo.shape
    rows = n_own + OWN_I
    full = nq // GROUP * GROUP
    me = lax.axis_index("pq")
    core = lax.axis_index("pb") & 1
    y = me & (NY - 1)
    half = pieces[0].shape[1]
    for k in range(NY):
        src = (y - k + NY) & (NY - 1)
        for c in range(2):
            shift = (core if c == 0 else 1 - core) * (n_own - half)
            for z in range(NZ):
                at = pl.multiple_of((z * NY + src) * n_own + shift, 8)
                tt[pl.ds(at, half), :] = pieces[2 * k + c][z]
    amps = tt[...]
    lp = jnp.dot(ov[...], amps, preferred_element_type=F32).reshape(nq, OWN_I, nocc)
    d[:, n_own:, :] = (lp + oo[...].astype(F32)).astype(BF16).astype(F32)

    def dress(t):
        q0, q1 = t * GROUP, min(nq, (t + 1) * GROUP)
        part = jnp.dot(vv[q0 * n_own : q1 * n_own, :], amps, preferred_element_type=F32)
        d[q0:q1, :n_own, :] = part.reshape(q1 - q0, n_own, nocc) + vo[q0:q1].astype(F32)

    left = nq - full
    spare = GROUP - left
    short = rows - 16

    def pack(t):
        for h in range(nocc // LANES):
            cols = slice(h * LANES, (h + 1) * LANES)
            for r in range(0, rows if t * GROUP < full else short, 8):
                if t * GROUP < full:
                    tiles = [d[t * GROUP + q, r : r + 8, cols] for q in range(GROUP)]
                else:
                    n, r2 = divmod(r, 16)
                    tiles = [d[full + q, r : r + 8, cols] for q in range(left)]
                    tiles += [
                        d[full + n * spare + v, short + r2 : short + r2 + 8, cols]
                        for v in range(spare)
                    ]
                for g, tile in enumerate(swap_blocks(tiles)):
                    out[h * GROUP + g, t * rows + r : t * rows + r + 8, :] = tile.astype(BF16)

    lane = lax.broadcasted_iota(jnp.int32, (1, LANES), 1)
    row = jnp.zeros((1, LANES), F32)
    n_tiles = -(-nq // GROUP)
    dress(0)
    for t in range(1, n_tiles):
        dress(t)
        pack(t - 1)
    gram[...] = lax.dot_general(amps, amps, TN, preferred_element_type=F32)
    pack(n_tiles - 1)
    weight = jnp.concatenate(
        [own[...].astype(F32), -gram[pl.ds(pl.multiple_of(me * OWN_I, 8), OWN_I), :]], 0
    )
    for q in range(nq):
        total = jnp.sum(d[q] * weight, axis=(0, 1), keepdims=True)
        row = jnp.where(lane == q, 2.0 * total, row)
    block = jnp.concatenate(
        [s.astype(F32) for s in split3(row)] + [jnp.zeros((8 - 3, LANES), F32)], 0
    ).astype(BF16)
    at = full // GROUP * rows + short
    for p in range(out.shape[0]):
        out[p, at : at + 8, :] = block


def receive_side(scale, got, tt, dressed, fock, raw, lpt):
    n_dev = got.shape[0]
    nq = dressed.shape[0] // OWN_I
    nvirt = tt.shape[0]
    n_own = nvirt // n_dev
    rows = n_own + OWN_I
    full = nq // GROUP * GROUP
    n_full = full // GROUP
    left = nq - full
    spare = GROUP - left
    short = rows - 16
    lane16 = lax.broadcasted_iota(jnp.int32, (16, LANES), 1)
    width = spare * OWN_I
    for p in range(n_dev):
        a = p * n_own
        for t in range(n_full):
            raw[a : a + n_own, t * LANES : (t + 1) * LANES] = got[p, t * rows : t * rows + n_own, :]
            lpt[p * OWN_I : (p + 1) * OWN_I, t * LANES : (t + 1) * LANES] = got[
                p, t * rows + n_own : (t + 1) * rows, :
            ]
        base = n_full * rows
        tail = jnp.zeros((16, LANES), F32)
        for n in range(short // 16):
            part = pltpu.roll(
                got[p, base + 16 * n : base + 16 * (n + 1), :].astype(F32), (n + 1) * width, 1
            )
            here = (lane16 >= n * width) & (lane16 < (n + 1) * width)
            tail = jnp.where(here, part, tail)
        raw[a : a + short, n_full * LANES :] = got[p, base : base + short, :]
        raw[a + short : a + n_own, n_full * LANES :] = tail[: n_own - short].astype(BF16)
        lpt[p * OWN_I : (p + 1) * OWN_I, n_full * LANES :] = tail[n_own - short :].astype(BF16)
    lanes_in = (n_full + 1) * LANES
    m = nq * OWN_I
    eye = (
        lax.broadcasted_iota(jnp.int32, (m, lanes_in), 0)
        == lax.broadcasted_iota(jnp.int32, (m, lanes_in), 1)
    ).astype(F32).astype(BF16)
    lp = lax.dot_general(eye, lpt[...], NT, preferred_element_type=F32).astype(BF16)
    moved = lax.dot_general(eye, raw[...], NT, preferred_element_type=F32)
    occupied = lax.dot_general(lp, tt[...], NT, preferred_element_type=F32)
    result = (moved - occupied).astype(BF16)
    dressed[...] = result
    at = n_full * rows + short
    shares = jnp.sum(got[:, at : at + 8, :].astype(F32), axis=0)
    coulomb = shares[0:1] + shares[1:2] + shares[2:3]
    pick = lax.broadcasted_iota(jnp.int32, (m, LANES), 1) == lax.broadcasted_iota(
        jnp.int32, (m, LANES), 0
    ) // OWN_I
    column = jnp.sum(jnp.where(pick, coulomb, 0.0), axis=1, keepdims=True)
    part = jnp.sum((column * result.astype(F32)).reshape(nq, OWN_I, nvirt), axis=0) * scale
    for copy in range(fock.shape[0]):
        fock[copy] = part.astype(fock.dtype)


VMEM = pl.BlockSpec(memory_space=pltpu.VMEM)
ANY = pl.BlockSpec(memory_space=pl.ANY)
FLOPS = 40_000_000_000
PARAMS = pltpu.CompilerParams(vmem_limit_bytes=26 * 1024 * 1024)


def per_device(chol_vv, chol_ov, chol_oo, chol_vo, amplitudes):
    nq, n_own, nvirt = chol_vv.shape
    nocc = amplitudes.shape[0]
    n_dev, n_pb = lax.axis_size("pq"), lax.axis_size("pb")
    own = amplitudes.T
    half = -(-n_own // 16) * 8
    copies = pl.pallas_call(
        spread,
        out_shape=jax.ShapeDtypeStruct((NZ, half, nocc), BF16),
        in_specs=[VMEM],
        out_specs=VMEM,
        compiler_params=PARAMS,
        cost_estimate=pl.CostEstimate(flops=FLOPS, bytes_accessed=0, transcendentals=0),
        name="spread",
    )(own)
    near = lax.all_to_all(copies, "pq", 0, 0, axis_index_groups=z_groups(), tiled=True)
    other = [(b, b ^ 1) for b in range(n_pb)]
    pieces = [near]
    for k in range(1, NY):
        pieces.append(lax.ppermute(near, "pq", y_shift(k)))
    pieces = [p for piece in pieces for p in (piece, lax.ppermute(piece, "pb", other))]
    blocks = (
        chol_vv.reshape(nq * n_own, nvirt),
        chol_ov.reshape(nq * OWN_I, nvirt),
        chol_oo,
        chol_vo.transpose(0, 2, 1),
    )
    token = pl.pallas_call(
        touch,
        out_shape=jax.ShapeDtypeStruct((8, LANES), F32),
        in_specs=[ANY] * 5,
        out_specs=VMEM,
        compiler_params=PARAMS,
        cost_estimate=pl.CostEstimate(flops=4_000_000_000, bytes_accessed=0, transcendentals=0),
        name="touch",
    )(near, *blocks)
    rows = n_own + OWN_I
    sent_rows = nq * rows * OWN_I // LANES + 8
    sent, tt = pl.pallas_call(
        send_side,
        out_shape=(
            jax.ShapeDtypeStruct((n_dev, sent_rows, LANES), BF16),
            jax.ShapeDtypeStruct((nvirt, nocc), BF16),
        ),
        in_specs=[ANY] + [VMEM] * (5 + 2 * NY),
        out_specs=(VMEM, VMEM),
        scratch_shapes=[pltpu.VMEM((nq, rows, nocc), F32), pltpu.VMEM((nocc, nocc), F32)],
        compiler_params=PARAMS,
        name="send_side",
    )(token, *blocks, own, *pieces)
    got = lax.all_to_all(sent, "pq", 0, 0, tiled=True)
    lanes_in = -(-nq // GROUP) * LANES
    dressed, fock = pl.pallas_call(
        functools.partial(receive_side, 1.0 / (nq * n_pb)),
        out_shape=(
            jax.ShapeDtypeStruct((nq * OWN_I, nvirt), BF16),
            jax.ShapeDtypeStruct((n_pb, OWN_I, nvirt), BF16),
        ),
        in_specs=[VMEM] * 2,
        out_specs=(VMEM, VMEM),
        scratch_shapes=[pltpu.VMEM((nvirt, lanes_in), BF16), pltpu.VMEM((nocc, lanes_in), BF16)],
        compiler_params=PARAMS,
        name="receive_side",
    )(got, tt)
    parts = lax.all_to_all(fock, "pb", 0, 0, tiled=True)
    fock_ov = jnp.sum(parts.astype(F32), axis=0)
    return dressed.reshape(nq, OWN_I, nvirt), fock_ov


def solution(mesh):
    in_specs = (
        P("pb", "pq", None),
        P("pb", "pq", None),
        P("pb", "pq", None),
        P("pb", None, "pq"),
        P(None, "pq"),
    )
    out_specs = (P("pb", "pq", None), P("pq", None))

    return jax.shard_map(
        per_device, mesh=mesh, in_specs=in_specs, out_specs=out_specs, check_vma=False
    )
```

```python
import functools

import jax
import jax.numpy as jnp
from jax import lax
from jax.experimental import pallas as pl
from jax.experimental.pallas import tpu as pltpu
from jax.sharding import PartitionSpec as P

NZ, NY = 8, 4
LANES = 128
OWN_I = 8
GROUP = LANES // OWN_I
F32, BF16 = jnp.float32, jnp.bfloat16
NT = (((1,), (1,)), ((), ()))
TN = (((0,), (0,)), ((), ()))


ORDER = [z * NY + y for y in range(NY) for z in range(NZ)]
PLACE = [ORDER.index(p) for p in range(NZ * NY)]


def z_groups():
    return [[z * NY + y for z in range(NZ)] for y in range(NY)]


def y_shift(k):
    return [(z * NY + y, z * NY + (y + k) % NY) for z in range(NZ) for y in range(NY)]


def split3(x):
    hi = x.astype(BF16)
    rest = x - hi.astype(F32)
    mid = rest.astype(BF16)
    low = (rest - mid.astype(F32)).astype(BF16)
    return hi, mid, low


def swap_blocks(tiles):
    lane = lax.broadcasted_iota(jnp.int32, tiles[0].shape, 1)
    bit = 1
    while bit < GROUP:
        upper = (lane // OWN_I) & bit != 0
        out = list(tiles)
        for q in range(GROUP):
            if q & bit:
                continue
            low, high = tiles[q], tiles[q | bit]
            out[q] = jnp.where(upper, pltpu.roll(high, OWN_I * bit, 1), low)
            out[q | bit] = jnp.where(upper, high, pltpu.roll(low, LANES - OWN_I * bit, 1))
        tiles = out
        bit *= 2
    return tiles


def spread(own, out):
    start = pl.multiple_of((lax.axis_index("pb") & 1) * LANES, LANES)
    part = own[:, pl.ds(start, LANES)]
    for copy in range(out.shape[0]):
        out[copy] = part


def touch(near, vv, ov, oo, vo, token):
    del near, vv, ov, oo, vo
    token[...] = jnp.zeros_like(token)


def send_side(token, vv, ov, oo, vo, own, *refs):
    del token
    pieces, (out, tt, d, gram) = refs[: 2 * NY], refs[2 * NY :]
    nq, n_own, nocc = vo.shape
    rows = n_own + OWN_I
    full = nq // GROUP * GROUP
    me = lax.axis_index("pq")
    core = lax.axis_index("pb") & 1
    y = me & (NY - 1)
    for k in range(NY):
        src = (y - k + NY) & (NY - 1)
        for c in range(2):
            cols = pl.multiple_of((core if c == 0 else 1 - core) * LANES, LANES)
            for z in range(NZ):
                at = pl.multiple_of((z * NY + src) * n_own, 8)
                tt[pl.ds(at, n_own), pl.ds(cols, LANES)] = pieces[2 * k + c][z]
    amps = tt[...]
    lp = jnp.dot(ov[...], amps, preferred_element_type=F32).reshape(nq, OWN_I, nocc)
    d[:, n_own:, :] = (lp + oo[...].astype(F32)).astype(BF16).astype(F32)

    def dress(t):
        q0, q1 = t * GROUP, min(nq, (t + 1) * GROUP)
        part = jnp.dot(vv[q0 * n_own : q1 * n_own, :], amps, preferred_element_type=F32)
        d[q0:q1, :n_own, :] = part.reshape(q1 - q0, n_own, nocc) + vo[q0:q1].astype(F32)

    left = nq - full
    spare = GROUP - left
    short = rows - 16

    def pack(t):
        for h in range(nocc // LANES):
            cols = slice(h * LANES, (h + 1) * LANES)
            for r in range(0, rows if t * GROUP < full else short, 8):
                if t * GROUP < full:
                    tiles = [d[t * GROUP + q, r : r + 8, cols] for q in range(GROUP)]
                else:
                    n, r2 = divmod(r, 16)
                    tiles = [d[full + q, r : r + 8, cols] for q in range(left)]
                    tiles += [
                        d[full + n * spare + v, short + r2 : short + r2 + 8, cols]
                        for v in range(spare)
                    ]
                for g, tile in enumerate(swap_blocks(tiles)):
                    out[PLACE[h * GROUP + g], t * rows + r : t * rows + r + 8, :] = tile.astype(BF16)

    lane = lax.broadcasted_iota(jnp.int32, (1, LANES), 1)
    row = jnp.zeros((1, LANES), F32)
    n_tiles = -(-nq // GROUP)
    dress(0)
    for t in range(1, n_tiles):
        dress(t)
        pack(t - 1)
    gram[...] = lax.dot_general(amps, amps, TN, preferred_element_type=F32)
    pack(n_tiles - 1)
    weight = jnp.concatenate(
        [own[...].astype(F32), -gram[pl.ds(pl.multiple_of(me * OWN_I, 8), OWN_I), :]], 0
    )
    for q in range(nq):
        total = jnp.sum(d[q] * weight, axis=(0, 1), keepdims=True)
        row = jnp.where(lane == q, 2.0 * total, row)
    block = jnp.concatenate(
        [s.astype(F32) for s in split3(row)] + [jnp.zeros((8 - 3, LANES), F32)], 0
    ).astype(BF16)
    at = full // GROUP * rows + short
    for p in range(out.shape[0]):
        out[p, at : at + 8, :] = block


def unpack(scale, got, tt, fock, raw, lpt):
    n_dev = got.shape[0]
    nvirt = tt.shape[0]
    n_own = nvirt // n_dev
    rows = n_own + OWN_I
    nq = (got.shape[1] - 8) * LANES // OWN_I // rows
    full = nq // GROUP * GROUP
    n_full = full // GROUP
    left = nq - full
    spare = GROUP - left
    short = rows - 16
    lane16 = lax.broadcasted_iota(jnp.int32, (16, LANES), 1)
    width = spare * OWN_I
    for p in range(n_dev):
        a, k = p * n_own, PLACE[p]
        for t in range(n_full):
            raw[a : a + n_own, t * LANES : (t + 1) * LANES] = got[k, t * rows : t * rows + n_own, :]
            lpt[p * OWN_I : (p + 1) * OWN_I, t * LANES : (t + 1) * LANES] = got[
                k, t * rows + n_own : (t + 1) * rows, :
            ]
        base = n_full * rows
        tail = jnp.zeros((16, LANES), F32)
        for n in range(short // 16):
            part = pltpu.roll(
                got[k, base + 16 * n : base + 16 * (n + 1), :].astype(F32), (n + 1) * width, 1
            )
            here = (lane16 >= n * width) & (lane16 < (n + 1) * width)
            tail = jnp.where(here, part, tail)
        raw[a : a + short, n_full * LANES :] = got[k, base : base + short, :]
        raw[a + short : a + n_own, n_full * LANES :] = tail[: n_own - short].astype(BF16)
        lpt[p * OWN_I : (p + 1) * OWN_I, n_full * LANES :] = tail[n_own - short :].astype(BF16)
    lanes_in = (n_full + 1) * LANES
    at = n_full * rows + short
    shares = jnp.sum(got[:, at : at + 8, :].astype(F32), axis=0)
    coulomb = jnp.broadcast_to((shares[0:1] + shares[1:2] + shares[2:3]) * scale, (OWN_I, LANES))
    column = lax.broadcasted_iota(jnp.int32, (LANES, lanes_in), 1)
    widen = (lax.broadcasted_iota(jnp.int32, (LANES, lanes_in), 0) == column // OWN_I).astype(F32).astype(BF16)
    column = lax.broadcasted_iota(jnp.int32, (OWN_I, lanes_in), 1)
    own_row = (column % OWN_I == lax.broadcasted_iota(jnp.int32, (OWN_I, lanes_in), 0)) & (
        column < nq * OWN_I
    )
    weight = jnp.concatenate(
        [
            jnp.where(own_row, jnp.dot(part, widen, preferred_element_type=F32), 0.0)
            for part in split3(coulomb)
        ],
        0,
    ).astype(BF16)

    def three(x):
        return x[:OWN_I] + x[OWN_I : 2 * OWN_I] + x[2 * OWN_I :]

    moved = three(lax.dot_general(weight, raw[...], NT, preferred_element_type=F32))
    lp = three(lax.dot_general(weight, lpt[...], NT, preferred_element_type=F32))
    lp = jnp.concatenate([part.astype(F32) for part in split3(lp)], 0).astype(BF16)
    part = moved - three(lax.dot_general(lp, tt[...], NT, preferred_element_type=F32))
    fock[...] = part


def both_cores(own, other, out):
    total = (own[...] + other[...]).astype(out.dtype)
    for copy in range(out.shape[0]):
        out[copy] = total


def dress(raw, lpt, tt, dressed):
    shape = (dressed.shape[0], raw.shape[1])
    eye = (
        lax.broadcasted_iota(jnp.int32, shape, 0) == lax.broadcasted_iota(jnp.int32, shape, 1)
    ).astype(F32).astype(BF16)
    lp = lax.dot_general(eye, lpt[...], NT, preferred_element_type=F32).astype(BF16)
    moved = lax.dot_general(eye, raw[...], NT, preferred_element_type=F32)
    occupied = lax.dot_general(lp, tt[...], NT, preferred_element_type=F32)
    dressed[...] = (moved - occupied).astype(BF16)


VMEM = pl.BlockSpec(memory_space=pltpu.VMEM)
ANY = pl.BlockSpec(memory_space=pl.ANY)
FLOPS = 40_000_000_000
PARAMS = pltpu.CompilerParams(vmem_limit_bytes=26 * 1024 * 1024)


def per_device(chol_vv, chol_ov, chol_oo, chol_vo, amplitudes):
    nq, n_own, nvirt = chol_vv.shape
    nocc = amplitudes.shape[0]
    n_dev, n_pb = lax.axis_size("pq"), lax.axis_size("pb")
    own = amplitudes.T
    copies = pl.pallas_call(
        spread,
        out_shape=jax.ShapeDtypeStruct((NZ, n_own, LANES), BF16),
        in_specs=[VMEM],
        out_specs=VMEM,
        compiler_params=PARAMS,
        cost_estimate=pl.CostEstimate(flops=FLOPS, bytes_accessed=0, transcendentals=0),
        name="spread",
    )(own)
    near = lax.all_to_all(copies, "pq", 0, 0, axis_index_groups=z_groups(), tiled=True)
    other = [(b, b ^ 1) for b in range(n_pb)]
    pieces = [near]
    for k in range(1, NY):
        pieces.append(lax.ppermute(near, "pq", y_shift(k)))
    pieces = [p for piece in pieces for p in (piece, lax.ppermute(piece, "pb", other))]
    blocks = (
        chol_vv.reshape(nq * n_own, nvirt),
        chol_ov.reshape(nq * OWN_I, nvirt),
        chol_oo,
        chol_vo.transpose(0, 2, 1),
    )
    token = pl.pallas_call(
        touch,
        out_shape=jax.ShapeDtypeStruct((8, LANES), F32),
        in_specs=[ANY] * 5,
        out_specs=VMEM,
        compiler_params=PARAMS,
        cost_estimate=pl.CostEstimate(flops=4_000_000_000, bytes_accessed=0, transcendentals=0),
        name="touch",
    )(near, *blocks)
    rows = n_own + OWN_I
    sent_rows = nq * rows * OWN_I // LANES + 8
    sent, tt = pl.pallas_call(
        send_side,
        out_shape=(
            jax.ShapeDtypeStruct((n_dev, sent_rows, LANES), BF16),
            jax.ShapeDtypeStruct((nvirt, nocc), BF16),
        ),
        in_specs=[ANY] + [VMEM] * (5 + 2 * NY),
        out_specs=(VMEM, VMEM),
        scratch_shapes=[pltpu.VMEM((nq, rows, nocc), F32), pltpu.VMEM((nocc, nocc), F32)],
        compiler_params=PARAMS,
        name="send_side",
    )(token, *blocks, own, *pieces)
    got = lax.all_to_all(sent, "pq", 0, 0, axis_index_groups=[ORDER], tiled=True)
    lanes_in = -(-nq // GROUP) * LANES
    fock, raw, lpt = pl.pallas_call(
        functools.partial(unpack, 1.0 / (nq * n_pb)),
        out_shape=(
            jax.ShapeDtypeStruct((OWN_I, nvirt), F32),
            jax.ShapeDtypeStruct((nvirt, lanes_in), BF16),
            jax.ShapeDtypeStruct((nocc, lanes_in), BF16),
        ),
        in_specs=[VMEM] * 2,
        out_specs=(VMEM,) * 3,
        compiler_params=PARAMS,
        name="unpack",
    )(got, tt)
    dressed = pl.pallas_call(
        dress,
        out_shape=jax.ShapeDtypeStruct((nq * OWN_I, nvirt), BF16),
        in_specs=[VMEM] * 3,
        out_specs=VMEM,
        compiler_params=PARAMS,
        cost_estimate=pl.CostEstimate(flops=FLOPS, bytes_accessed=0, transcendentals=0),
        name="dress",
    )(raw, lpt, tt)
    partner = lax.ppermute(fock, "pb", other)
    halves = pl.pallas_call(
        both_cores,
        out_shape=jax.ShapeDtypeStruct((n_pb // 2, OWN_I, nvirt), BF16),
        in_specs=[VMEM] * 2,
        out_specs=VMEM,
        compiler_params=PARAMS,
        name="both_cores",
    )(fock, partner)
    x_groups = [list(range(c, n_pb, 2)) for c in range(2)]
    parts = lax.all_to_all(halves, "pb", 0, 0, axis_index_groups=x_groups, tiled=True)
    fock_ov = jnp.sum(parts.astype(F32), axis=0)
    return dressed.reshape(nq, OWN_I, nvirt), fock_ov


def solution(mesh):
    in_specs = (
        P("pb", "pq", None),
        P("pb", "pq", None),
        P("pb", "pq", None),
        P("pb", None, "pq"),
        P(None, "pq"),
    )
    out_specs = (P("pb", "pq", None), P("pq", None))

    return jax.shard_map(per_device, mesh=mesh, in_specs=in_specs, out_specs=out_specs, check_vma=False)
```

```python
import functools

import jax
import jax.numpy as jnp
from jax import lax
from jax.experimental import pallas as pl
from jax.experimental.pallas import tpu as pltpu
from jax.sharding import PartitionSpec as P

NZ, NY = 8, 4
LANES = 128
OWN_I = 8
GROUP = LANES // OWN_I
F32, BF16 = jnp.float32, jnp.bfloat16
NT = (((1,), (1,)), ((), ()))
TN = (((0,), (0,)), ((), ()))


Z_ORDER = list(reversed(range(NZ)))
ORDER = [z * NY + y for y in range(NY) for z in reversed(range(NZ))]
PLACE = [ORDER.index(p) for p in range(NZ * NY)]


def z_groups():
    return [[z * NY + y for z in Z_ORDER] for y in range(NY)]


def y_shift(k):
    return [(z * NY + y, z * NY + (y + k) % NY) for z in range(NZ) for y in range(NY)]


def split3(x):
    hi = x.astype(BF16)
    rest = x - hi.astype(F32)
    mid = rest.astype(BF16)
    low = (rest - mid.astype(F32)).astype(BF16)
    return hi, mid, low


def swap_blocks(tiles):
    lane = lax.broadcasted_iota(jnp.int32, tiles[0].shape, 1)
    bit = 1
    while bit < GROUP:
        upper = (lane // OWN_I) & bit != 0
        out = list(tiles)
        for q in range(GROUP):
            if q & bit:
                continue
            low, high = tiles[q], tiles[q | bit]
            out[q] = jnp.where(upper, pltpu.roll(high, OWN_I * bit, 1), low)
            out[q | bit] = jnp.where(upper, high, pltpu.roll(low, LANES - OWN_I * bit, 1))
        tiles = out
        bit *= 2
    return tiles


def spread(own, out):
    start = pl.multiple_of((lax.axis_index("pb") & 1) * LANES, LANES)
    part = own[:, pl.ds(start, LANES)]
    for copy in range(out.shape[0]):
        out[copy] = part


def touch(near, vv, ov, oo, vo, token):
    del near, vv, ov, oo, vo
    token[...] = jnp.zeros_like(token)


def send_side(token, vv, ov, oo, vo, own, *refs):
    del token
    pieces, (out, tt, d, gram) = refs[: 2 * NY], refs[2 * NY :]
    nq, n_own, nocc = vo.shape
    rows = n_own + OWN_I
    full = nq // GROUP * GROUP
    me = lax.axis_index("pq")
    core = lax.axis_index("pb") & 1
    y = me & (NY - 1)
    for k in range(NY):
        src = (y - k + NY) & (NY - 1)
        for c in range(2):
            cols = pl.multiple_of((core if c == 0 else 1 - core) * LANES, LANES)
            for k_z, z in enumerate(Z_ORDER):
                at = pl.multiple_of((z * NY + src) * n_own, 8)
                tt[pl.ds(at, n_own), pl.ds(cols, LANES)] = pieces[2 * k + c][k_z]
    amps = tt[...]
    lp = jnp.dot(ov[...], amps, preferred_element_type=F32).reshape(nq, OWN_I, nocc)
    d[:, n_own:, :] = (lp + oo[...].astype(F32)).astype(BF16).astype(F32)

    def dress(t):
        q0, q1 = t * GROUP, min(nq, (t + 1) * GROUP)
        part = jnp.dot(vv[q0 * n_own : q1 * n_own, :], amps, preferred_element_type=F32)
        d[q0:q1, :n_own, :] = part.reshape(q1 - q0, n_own, nocc) + vo[q0:q1].astype(F32)

    left = nq - full
    spare = GROUP - left
    short = rows - 16

    def pack(t):
        for h in range(nocc // LANES):
            cols = slice(h * LANES, (h + 1) * LANES)
            for r in range(0, rows if t * GROUP < full else short, 8):
                if t * GROUP < full:
                    tiles = [d[t * GROUP + q, r : r + 8, cols] for q in range(GROUP)]
                else:
                    n, r2 = divmod(r, 16)
                    tiles = [d[full + q, r : r + 8, cols] for q in range(left)]
                    tiles += [
                        d[full + n * spare + v, short + r2 : short + r2 + 8, cols]
                        for v in range(spare)
                    ]
                for g, tile in enumerate(swap_blocks(tiles)):
                    out[PLACE[h * GROUP + g], t * rows + r : t * rows + r + 8, :] = tile.astype(BF16)

    lane = lax.broadcasted_iota(jnp.int32, (1, LANES), 1)
    row = jnp.zeros((1, LANES), F32)
    n_tiles = -(-nq // GROUP)
    dress(0)
    for t in range(1, n_tiles):
        dress(t)
        pack(t - 1)
    gram[...] = lax.dot_general(amps, amps, TN, preferred_element_type=F32)
    pack(n_tiles - 1)
    weight = jnp.concatenate(
        [own[...].astype(F32), -gram[pl.ds(pl.multiple_of(me * OWN_I, 8), OWN_I), :]], 0
    )
    for q in range(nq):
        total = jnp.sum(d[q] * weight, axis=(0, 1), keepdims=True)
        row = jnp.where(lane == q, 2.0 * total, row)
    block = jnp.concatenate(
        [s.astype(F32) for s in split3(row)] + [jnp.zeros((8 - 3, LANES), F32)], 0
    ).astype(BF16)
    at = full // GROUP * rows + short
    for p in range(out.shape[0]):
        out[p, at : at + 8, :] = block


def unpack(scale, got, tt, fock, raw, lpt):
    n_dev = got.shape[0]
    nvirt = tt.shape[0]
    n_own = nvirt // n_dev
    rows = n_own + OWN_I
    nq = (got.shape[1] - 8) * LANES // OWN_I // rows
    full = nq // GROUP * GROUP
    n_full = full // GROUP
    left = nq - full
    spare = GROUP - left
    short = rows - 16
    lane16 = lax.broadcasted_iota(jnp.int32, (16, LANES), 1)
    width = spare * OWN_I
    for p in range(n_dev):
        a, k = p * n_own, PLACE[p]
        for t in range(n_full):
            raw[a : a + n_own, t * LANES : (t + 1) * LANES] = got[k, t * rows : t * rows + n_own, :]
            lpt[p * OWN_I : (p + 1) * OWN_I, t * LANES : (t + 1) * LANES] = got[
                k, t * rows + n_own : (t + 1) * rows, :
            ]
        base = n_full * rows
        tail = jnp.zeros((16, LANES), F32)
        for n in range(short // 16):
            part = pltpu.roll(
                got[k, base + 16 * n : base + 16 * (n + 1), :].astype(F32), (n + 1) * width, 1
            )
            here = (lane16 >= n * width) & (lane16 < (n + 1) * width)
            tail = jnp.where(here, part, tail)
        raw[a : a + short, n_full * LANES :] = got[k, base : base + short, :]
        raw[a + short : a + n_own, n_full * LANES :] = tail[: n_own - short].astype(BF16)
        lpt[p * OWN_I : (p + 1) * OWN_I, n_full * LANES :] = tail[n_own - short :].astype(BF16)
    lanes_in = (n_full + 1) * LANES
    at = n_full * rows + short
    shares = jnp.sum(got[:, at : at + 8, :].astype(F32), axis=0)
    coulomb = jnp.broadcast_to((shares[0:1] + shares[1:2] + shares[2:3]) * scale, (OWN_I, LANES))
    column = lax.broadcasted_iota(jnp.int32, (LANES, lanes_in), 1)
    widen = (lax.broadcasted_iota(jnp.int32, (LANES, lanes_in), 0) == column // OWN_I).astype(F32).astype(BF16)
    column = lax.broadcasted_iota(jnp.int32, (OWN_I, lanes_in), 1)
    own_row = (column % OWN_I == lax.broadcasted_iota(jnp.int32, (OWN_I, lanes_in), 0)) & (
        column < nq * OWN_I
    )
    weight = jnp.concatenate(
        [
            jnp.where(own_row, jnp.dot(part, widen, preferred_element_type=F32), 0.0)
            for part in split3(coulomb)
        ],
        0,
    ).astype(BF16)

    def three(x):
        return x[:OWN_I] + x[OWN_I : 2 * OWN_I] + x[2 * OWN_I :]

    moved = three(lax.dot_general(weight, raw[...], NT, preferred_element_type=F32))
    lp = three(lax.dot_general(weight, lpt[...], NT, preferred_element_type=F32))
    lp = jnp.concatenate([part.astype(F32) for part in split3(lp)], 0).astype(BF16)
    part = moved - three(lax.dot_general(lp, tt[...], NT, preferred_element_type=F32))
    fock[...] = part


def both_cores(own, other, out):
    total = (own[...] + other[...]).astype(out.dtype)
    for copy in range(out.shape[0]):
        out[copy] = total


def dress(raw, lpt, tt, dressed):
    shape = (dressed.shape[0], raw.shape[1])
    eye = (
        lax.broadcasted_iota(jnp.int32, shape, 0) == lax.broadcasted_iota(jnp.int32, shape, 1)
    ).astype(F32).astype(BF16)
    lp = lax.dot_general(eye, lpt[...], NT, preferred_element_type=F32).astype(BF16)
    moved = lax.dot_general(eye, raw[...], NT, preferred_element_type=F32)
    occupied = lax.dot_general(lp, tt[...], NT, preferred_element_type=F32)
    dressed[...] = (moved - occupied).astype(BF16)


VMEM = pl.BlockSpec(memory_space=pltpu.VMEM)
ANY = pl.BlockSpec(memory_space=pl.ANY)
FLOPS = 40_000_000_000
PARAMS = pltpu.CompilerParams(vmem_limit_bytes=26 * 1024 * 1024)


def per_device(chol_vv, chol_ov, chol_oo, chol_vo, amplitudes):
    nq, n_own, nvirt = chol_vv.shape
    nocc = amplitudes.shape[0]
    n_dev, n_pb = lax.axis_size("pq"), lax.axis_size("pb")
    own = amplitudes.T
    copies = pl.pallas_call(
        spread,
        out_shape=jax.ShapeDtypeStruct((NZ, n_own, LANES), BF16),
        in_specs=[VMEM],
        out_specs=VMEM,
        compiler_params=PARAMS,
        cost_estimate=pl.CostEstimate(flops=FLOPS, bytes_accessed=0, transcendentals=0),
        name="spread",
    )(own)
    near = lax.all_to_all(copies, "pq", 0, 0, axis_index_groups=z_groups(), tiled=True)
    other = [(b, b ^ 1) for b in range(n_pb)]
    pieces = [near]
    for k in range(1, NY):
        pieces.append(lax.ppermute(near, "pq", y_shift(k)))
    pieces = [p for piece in pieces for p in (piece, lax.ppermute(piece, "pb", other))]
    blocks = (
        chol_vv.reshape(nq * n_own, nvirt),
        chol_ov.reshape(nq * OWN_I, nvirt),
        chol_oo,
        chol_vo.transpose(0, 2, 1),
    )
    token = pl.pallas_call(
        touch,
        out_shape=jax.ShapeDtypeStruct((8, LANES), F32),
        in_specs=[ANY] * 5,
        out_specs=VMEM,
        compiler_params=PARAMS,
        cost_estimate=pl.CostEstimate(flops=4_000_000_000, bytes_accessed=0, transcendentals=0),
        name="touch",
    )(near, *blocks)
    rows = n_own + OWN_I
    sent_rows = nq * rows * OWN_I // LANES + 8
    sent, tt = pl.pallas_call(
        send_side,
        out_shape=(
            jax.ShapeDtypeStruct((n_dev, sent_rows, LANES), BF16),
            jax.ShapeDtypeStruct((nvirt, nocc), BF16),
        ),
        in_specs=[ANY] + [VMEM] * (5 + 2 * NY),
        out_specs=(VMEM, VMEM),
        scratch_shapes=[pltpu.VMEM((nq, rows, nocc), F32), pltpu.VMEM((nocc, nocc), F32)],
        compiler_params=PARAMS,
        name="send_side",
    )(token, *blocks, own, *pieces)
    got = lax.all_to_all(sent, "pq", 0, 0, axis_index_groups=[ORDER], tiled=True)
    lanes_in = -(-nq // GROUP) * LANES
    fock, raw, lpt = pl.pallas_call(
        functools.partial(unpack, 1.0 / (nq * n_pb)),
        out_shape=(
            jax.ShapeDtypeStruct((OWN_I, nvirt), F32),
            jax.ShapeDtypeStruct((nvirt, lanes_in), BF16),
            jax.ShapeDtypeStruct((nocc, lanes_in), BF16),
        ),
        in_specs=[VMEM] * 2,
        out_specs=(VMEM,) * 3,
        compiler_params=PARAMS,
        name="unpack",
    )(got, tt)
    dressed = pl.pallas_call(
        dress,
        out_shape=jax.ShapeDtypeStruct((nq * OWN_I, nvirt), BF16),
        in_specs=[VMEM] * 3,
        out_specs=VMEM,
        compiler_params=PARAMS,
        cost_estimate=pl.CostEstimate(flops=FLOPS, bytes_accessed=0, transcendentals=0),
        name="dress",
    )(raw, lpt, tt)
    partner = lax.ppermute(fock, "pb", other)
    halves = pl.pallas_call(
        both_cores,
        out_shape=jax.ShapeDtypeStruct((n_pb // 2, OWN_I, nvirt), BF16),
        in_specs=[VMEM] * 2,
        out_specs=VMEM,
        compiler_params=PARAMS,
        name="both_cores",
    )(fock, partner)
    x_groups = [list(range(c, n_pb, 2)) for c in range(2)]
    parts = lax.all_to_all(halves, "pb", 0, 0, axis_index_groups=x_groups, tiled=True)
    fock_ov = jnp.sum(parts.astype(F32), axis=0)
    return dressed.reshape(nq, OWN_I, nvirt), fock_ov


def solution(mesh):
    in_specs = (
        P("pb", "pq", None),
        P("pb", "pq", None),
        P("pb", "pq", None),
        P("pb", None, "pq"),
        P(None, "pq"),
    )
    out_specs = (P("pb", "pq", None), P("pq", None))

    return jax.shard_map(per_device, mesh=mesh, in_specs=in_specs, out_specs=out_specs, check_vma=False)
```

```python
import functools

import jax
import jax.numpy as jnp
from jax import lax
from jax.experimental import pallas as pl
from jax.experimental.pallas import tpu as pltpu
from jax.sharding import PartitionSpec as P

NZ, NY = 8, 4
LANES = 128
OWN_I = 8
GROUP = LANES // OWN_I
F32, BF16 = jnp.float32, jnp.bfloat16
NT = (((1,), (1,)), ((), ()))
TN = (((0,), (0,)), ((), ()))


Z_ORDER = list(reversed(range(NZ)))
ORDER = [z * NY + y for z in reversed(range(NZ)) for y in range(NY)]
PLACE = [ORDER.index(p) for p in range(NZ * NY)]


def z_groups():
    return [[z * NY + y for z in Z_ORDER] for y in range(NY)]


def y_shift(k):
    return [(z * NY + y, z * NY + (y + k) % NY) for z in range(NZ) for y in range(NY)]


def split3(x):
    hi = x.astype(BF16)
    rest = x - hi.astype(F32)
    mid = rest.astype(BF16)
    low = (rest - mid.astype(F32)).astype(BF16)
    return hi, mid, low


def swap_blocks(tiles):
    lane = lax.broadcasted_iota(jnp.int32, tiles[0].shape, 1)
    bit = 1
    while bit < GROUP:
        upper = (lane // OWN_I) & bit != 0
        out = list(tiles)
        for q in range(GROUP):
            if q & bit:
                continue
            low, high = tiles[q], tiles[q | bit]
            out[q] = jnp.where(upper, pltpu.roll(high, OWN_I * bit, 1), low)
            out[q | bit] = jnp.where(upper, high, pltpu.roll(low, LANES - OWN_I * bit, 1))
        tiles = out
        bit *= 2
    return tiles


def spread(own, out):
    start = pl.multiple_of((lax.axis_index("pb") & 1) * LANES, LANES)
    part = own[:, pl.ds(start, LANES)]
    for copy in range(out.shape[0]):
        out[copy] = part


def touch(near, vv, ov, oo, vo, token):
    del near, vv, ov, oo, vo
    token[...] = jnp.zeros_like(token)


def send_side(token, vv, ov, oo, vo, own, *refs):
    del token
    pieces, (out, tt, d, gram) = refs[: 2 * NY], refs[2 * NY :]
    nq, n_own, nocc = vo.shape
    rows = n_own + OWN_I
    full = nq // GROUP * GROUP
    me = lax.axis_index("pq")
    core = lax.axis_index("pb") & 1
    y = me & (NY - 1)
    for k in range(NY):
        src = (y + k) & (NY - 1)
        for c in range(2):
            cols = pl.multiple_of((core if c == 0 else 1 - core) * LANES, LANES)
            for k_z, z in enumerate(Z_ORDER):
                at = pl.multiple_of((z * NY + src) * n_own, 8)
                tt[pl.ds(at, n_own), pl.ds(cols, LANES)] = pieces[2 * k + c][k_z]
    amps = tt[...]
    lp = jnp.dot(ov[...], amps, preferred_element_type=F32).reshape(nq, OWN_I, nocc)
    d[:, n_own:, :] = (lp + oo[...].astype(F32)).astype(BF16).astype(F32)

    def dress(t):
        q0, q1 = t * GROUP, min(nq, (t + 1) * GROUP)
        part = jnp.dot(vv[q0 * n_own : q1 * n_own, :], amps, preferred_element_type=F32)
        d[q0:q1, :n_own, :] = part.reshape(q1 - q0, n_own, nocc) + vo[q0:q1].astype(F32)

    left = nq - full
    spare = GROUP - left
    short = rows - 16

    def pack(t):
        for h in range(nocc // LANES):
            cols = slice(h * LANES, (h + 1) * LANES)
            for r in range(0, rows if t * GROUP < full else short, 8):
                if t * GROUP < full:
                    tiles = [d[t * GROUP + q, r : r + 8, cols] for q in range(GROUP)]
                else:
                    n, r2 = divmod(r, 16)
                    tiles = [d[full + q, r : r + 8, cols] for q in range(left)]
                    tiles += [
                        d[full + n * spare + v, short + r2 : short + r2 + 8, cols]
                        for v in range(spare)
                    ]
                for g, tile in enumerate(swap_blocks(tiles)):
                    out[PLACE[h * GROUP + g], t * rows + r : t * rows + r + 8, :] = tile.astype(BF16)

    lane = lax.broadcasted_iota(jnp.int32, (1, LANES), 1)
    row = jnp.zeros((1, LANES), F32)
    n_tiles = -(-nq // GROUP)
    dress(0)
    for t in range(1, n_tiles):
        dress(t)
        pack(t - 1)
    gram[...] = lax.dot_general(amps, amps, TN, preferred_element_type=F32)
    pack(n_tiles - 1)
    weight = jnp.concatenate(
        [own[...].astype(F32), -gram[pl.ds(pl.multiple_of(me * OWN_I, 8), OWN_I), :]], 0
    )
    for q in range(nq):
        total = jnp.sum(d[q] * weight, axis=(0, 1), keepdims=True)
        row = jnp.where(lane == q, 2.0 * total, row)
    block = jnp.concatenate(
        [s.astype(F32) for s in split3(row)] + [jnp.zeros((8 - 3, LANES), F32)], 0
    ).astype(BF16)
    at = full // GROUP * rows + short
    for p in range(out.shape[0]):
        out[p, at : at + 8, :] = block


def unpack(scale, got, tt, fock, raw, lpt):
    n_dev = got.shape[0]
    nvirt = tt.shape[0]
    n_own = nvirt // n_dev
    rows = n_own + OWN_I
    nq = (got.shape[1] - 8) * LANES // OWN_I // rows
    full = nq // GROUP * GROUP
    n_full = full // GROUP
    left = nq - full
    spare = GROUP - left
    short = rows - 16
    lane16 = lax.broadcasted_iota(jnp.int32, (16, LANES), 1)
    width = spare * OWN_I
    for p in range(n_dev):
        a, k = p * n_own, PLACE[p]
        for t in range(n_full):
            raw[a : a + n_own, t * LANES : (t + 1) * LANES] = got[k, t * rows : t * rows + n_own, :]
            lpt[p * OWN_I : (p + 1) * OWN_I, t * LANES : (t + 1) * LANES] = got[
                k, t * rows + n_own : (t + 1) * rows, :
            ]
        base = n_full * rows
        tail = jnp.zeros((16, LANES), F32)
        for n in range(short // 16):
            part = pltpu.roll(
                got[k, base + 16 * n : base + 16 * (n + 1), :].astype(F32), (n + 1) * width, 1
            )
            here = (lane16 >= n * width) & (lane16 < (n + 1) * width)
            tail = jnp.where(here, part, tail)
        raw[a : a + short, n_full * LANES :] = got[k, base : base + short, :]
        raw[a + short : a + n_own, n_full * LANES :] = tail[: n_own - short].astype(BF16)
        lpt[p * OWN_I : (p + 1) * OWN_I, n_full * LANES :] = tail[n_own - short :].astype(BF16)
    lanes_in = (n_full + 1) * LANES
    at = n_full * rows + short
    shares = jnp.sum(got[:, at : at + 8, :].astype(F32), axis=0)
    coulomb = jnp.broadcast_to((shares[0:1] + shares[1:2] + shares[2:3]) * scale, (OWN_I, LANES))
    column = lax.broadcasted_iota(jnp.int32, (LANES, lanes_in), 1)
    widen = (lax.broadcasted_iota(jnp.int32, (LANES, lanes_in), 0) == column // OWN_I).astype(F32).astype(BF16)
    column = lax.broadcasted_iota(jnp.int32, (OWN_I, lanes_in), 1)
    own_row = (column % OWN_I == lax.broadcasted_iota(jnp.int32, (OWN_I, lanes_in), 0)) & (
        column < nq * OWN_I
    )
    weight = jnp.concatenate(
        [
            jnp.where(own_row, jnp.dot(part, widen, preferred_element_type=F32), 0.0)
            for part in split3(coulomb)
        ],
        0,
    ).astype(BF16)

    def three(x):
        return x[:OWN_I] + x[OWN_I : 2 * OWN_I] + x[2 * OWN_I :]

    moved = three(lax.dot_general(weight, raw[...], NT, preferred_element_type=F32))
    lp = three(lax.dot_general(weight, lpt[...], NT, preferred_element_type=F32))
    lp = jnp.concatenate([part.astype(F32) for part in split3(lp)], 0).astype(BF16)
    part = moved - three(lax.dot_general(lp, tt[...], NT, preferred_element_type=F32))
    fock[...] = part


def both_cores(own, other, out):
    total = (own[...] + other[...]).astype(out.dtype)
    for copy in range(out.shape[0]):
        out[copy] = total


def dress(raw, lpt, tt, dressed):
    shape = (dressed.shape[0], raw.shape[1])
    eye = (
        lax.broadcasted_iota(jnp.int32, shape, 0) == lax.broadcasted_iota(jnp.int32, shape, 1)
    ).astype(F32).astype(BF16)
    lp = lax.dot_general(eye, lpt[...], NT, preferred_element_type=F32).astype(BF16)
    moved = lax.dot_general(eye, raw[...], NT, preferred_element_type=F32)
    occupied = lax.dot_general(lp, tt[...], NT, preferred_element_type=F32)
    dressed[...] = (moved - occupied).astype(BF16)


VMEM = pl.BlockSpec(memory_space=pltpu.VMEM)
ANY = pl.BlockSpec(memory_space=pl.ANY)
FLOPS = 40_000_000_000
PARAMS = pltpu.CompilerParams(vmem_limit_bytes=26 * 1024 * 1024)


def per_device(chol_vv, chol_ov, chol_oo, chol_vo, amplitudes):
    nq, n_own, nvirt = chol_vv.shape
    nocc = amplitudes.shape[0]
    n_dev, n_pb = lax.axis_size("pq"), lax.axis_size("pb")
    own = amplitudes.T
    copies = pl.pallas_call(
        spread,
        out_shape=jax.ShapeDtypeStruct((NZ, n_own, LANES), BF16),
        in_specs=[VMEM],
        out_specs=VMEM,
        compiler_params=PARAMS,
        cost_estimate=pl.CostEstimate(flops=FLOPS, bytes_accessed=0, transcendentals=0),
        name="spread",
    )(own)
    near = lax.all_to_all(copies, "pq", 0, 0, axis_index_groups=z_groups(), tiled=True)
    other = [(b, b ^ 1) for b in range(n_pb)]
    pieces = [near]
    for k in range(1, NY):
        pieces.append(lax.ppermute(near, "pq", y_shift(NY - k)))
    pieces = [p for piece in pieces for p in (piece, lax.ppermute(piece, "pb", other))]
    blocks = (
        chol_vv.reshape(nq * n_own, nvirt),
        chol_ov.reshape(nq * OWN_I, nvirt),
        chol_oo,
        chol_vo.transpose(0, 2, 1),
    )
    token = pl.pallas_call(
        touch,
        out_shape=jax.ShapeDtypeStruct((8, LANES), F32),
        in_specs=[ANY] * 5,
        out_specs=VMEM,
        compiler_params=PARAMS,
        cost_estimate=pl.CostEstimate(flops=4_000_000_000, bytes_accessed=0, transcendentals=0),
        name="touch",
    )(near, *blocks)
    rows = n_own + OWN_I
    sent_rows = nq * rows * OWN_I // LANES + 8
    sent, tt = pl.pallas_call(
        send_side,
        out_shape=(
            jax.ShapeDtypeStruct((n_dev, sent_rows, LANES), BF16),
            jax.ShapeDtypeStruct((nvirt, nocc), BF16),
        ),
        in_specs=[ANY] + [VMEM] * (5 + 2 * NY),
        out_specs=(VMEM, VMEM),
        scratch_shapes=[pltpu.VMEM((nq, rows, nocc), F32), pltpu.VMEM((nocc, nocc), F32)],
        compiler_params=PARAMS,
        name="send_side",
    )(token, *blocks, own, *pieces)
    got = lax.all_to_all(sent, "pq", 0, 0, axis_index_groups=[ORDER], tiled=True)
    lanes_in = -(-nq // GROUP) * LANES
    fock, raw, lpt = pl.pallas_call(
        functools.partial(unpack, 1.0 / (nq * n_pb)),
        out_shape=(
            jax.ShapeDtypeStruct((OWN_I, nvirt), F32),
            jax.ShapeDtypeStruct((nvirt, lanes_in), BF16),
            jax.ShapeDtypeStruct((nocc, lanes_in), BF16),
        ),
        in_specs=[VMEM] * 2,
        out_specs=(VMEM,) * 3,
        compiler_params=PARAMS,
        name="unpack",
    )(got, tt)
    dressed = pl.pallas_call(
        dress,
        out_shape=jax.ShapeDtypeStruct((nq * OWN_I, nvirt), BF16),
        in_specs=[VMEM] * 3,
        out_specs=VMEM,
        compiler_params=PARAMS,
        cost_estimate=pl.CostEstimate(flops=FLOPS, bytes_accessed=0, transcendentals=0),
        name="dress",
    )(raw, lpt, tt)
    partner = lax.ppermute(fock, "pb", other)
    halves = pl.pallas_call(
        both_cores,
        out_shape=jax.ShapeDtypeStruct((n_pb // 2, OWN_I, nvirt), BF16),
        in_specs=[VMEM] * 2,
        out_specs=VMEM,
        compiler_params=PARAMS,
        name="both_cores",
    )(fock, partner)
    x_groups = [list(range(c, n_pb, 2))[::-1] for c in range(2)]
    parts = lax.all_to_all(halves, "pb", 0, 0, axis_index_groups=x_groups, tiled=True)
    fock_ov = jnp.sum(parts.astype(F32), axis=0)
    return dressed.reshape(nq, OWN_I, nvirt), fock_ov


def solution(mesh):
    in_specs = (
        P("pb", "pq", None),
        P("pb", "pq", None),
        P("pb", "pq", None),
        P("pb", None, "pq"),
        P(None, "pq"),
    )
    out_specs = (P("pb", "pq", None), P("pq", None))

    return jax.shard_map(per_device, mesh=mesh, in_specs=in_specs, out_specs=out_specs, check_vma=False)
```
